32 devices in a mesh: tm: 4 (over y, core), lat: 8 (over z, x).
Axes of the slice: x: 2, y: 2, z: 4, core: 2. Of those that a mesh axis runs over, the one named last changes fastest.
Arguments:
- trajectory: float32 [4, 32, 64, 2048], P('tm', 'lat'), may hold values from -6 to 6
- diffusivity: float32 [4, 32, 64, 2048], P('tm', 'lat'), may hold values from 0.02 to 0.24
- adjoint_end: bfloat16 [32, 64, 2048], P('lat'), may hold values from -6 to 6
- obs_jac: bfloat16 [3072, 128, 128], P(('tm', 'lat')), may hold values from -0.5 to 0.5
- obs_value: float32 [3072, 128], P(('tm', 'lat')), may hold values from -6 to 6
- obs_weight: float32 [3072, 128], P(('tm', 'lat')), may hold values from 0.3 to 3
- obs_valid: int32 [3072, 128], P(('tm', 'lat')), may hold values 0 or 1
- obs_owner: int32 [3072, 1], P(('tm', 'lat')), may hold values from 0 to 31; in each aligned block of 96 rows (0 to 95, 96 to 191, ...) at most 6 rows name the same one
- obs_tile: int32 [3072], P(('tm', 'lat')), may hold values from 0 to 4095
Outputs:
- adjoint: float32 [4, 32, 64, 2048], P('tm', 'lat')
The draws below stay inside these ranges and needn't reach their ends.
Inputs may be any that keep to these rules, and one draw needn't show every extreme that they name: `obs_owner`: among the 96 blocks of one device, no owner is named more than 6 times, a bound that some block reaches.
All inputs are finite; a program needn't handle non-finite values. No bound on the sum of `obs_valid` on one device may be relied on, other than what follows from the above.
Results may differ from the reference program's by a relative error of at most 0.0024.
Values may be sent and summed in bfloat16 or wider, within the bound.
No kernel may reach another device: no remote copies, remote signals or barrier semaphores. Data moves between devices by JAX's collectives and lax.ppermute only.
A program may use at most 128 MiB of HBM per device.

```python
import math
import jax
import jax.numpy as jnp
import numpy as np
from jax import lax

NLON = 2048
LEV = 64
TW = 2
CH = 128
SUB = 2
NB_DEV = 96
SECTIONS = 4
NLAT = 32
TILE = 128
TILES_DEV = 4096
CAP = 6
NOBS = 3072
N_LAT = 8
DEVICES = 32


def with_ends(entries, key, smallest, high):
    shape = entries.shape
    place = [jax.random.randint(jax.random.fold_in(key, axis), (), 0, shape[axis]) for axis in range(len(shape))]
    entries = entries.at[tuple(place)].set(smallest)
    longest = shape.index(max(shape))
    place[longest] = (place[longest] + 1) % shape[longest]
    return entries.at[tuple(place)].set(high)


def block_levels(rng, shape, cuts, least, largest):
    def one(dim, parts):
        draws = jax.random.uniform(jax.random.fold_in(jax.random.fold_in(rng, 6), dim), (parts,), jnp.float32, least / len(cuts), largest / len(cuts))
        return jnp.repeat(jnp.exp(draws), shape[dim] // parts).reshape((-1,) + (1,) * (len(shape) - dim - 1))

    loudness = one(*cuts[0])
    for cut in cuts[1:]:
        loudness = loudness * one(*cut)
    return loudness


def deal_out(key, own, number, rows, count, top, most, lean):
    sequence = jax.random.permutation(key, count)
    packed, ordinary = load_shares(count, rows * top, most, lean, True), load_shares(count, rows * top, most, lean, False)
    places = jnp.arange(count)

    def named(tallies, rotation):
        used = int((tallies > 0).sum())
        fixed = max(1, used // 4)
        shifted = fixed + (places - fixed + rotation * (used - fixed)) % max(1, count - fixed)
        return jnp.zeros((count,), jnp.int32).at[sequence[jnp.where(places < fixed, places, shifted)]].set(jnp.asarray(tallies, jnp.int32))

    tallies = jnp.where(number % 4 == 0, named(packed, number // 4), named(ordinary, number - number // 4 - 1))
    mixed = jax.random.permutation(jax.random.fold_in(own, 3), count)
    source_of, sink = mixed[0:count // 2 * 2:2], mixed[1:count // 2 * 2:2]
    slack = jnp.minimum(tallies[source_of] - 1, most - tallies[sink]) // 2
    slack = jnp.where((source_of == sequence[0]) | (sink == sequence[0]) | (tallies[sink] == 0), 0, jnp.maximum(slack, 0))
    shifted = jax.random.randint(jax.random.fold_in(own, 4), (count // 2,), 0, 1 << 20) % (slack + 1)
    tallies = tallies.at[source_of].add(-shifted).at[sink].add(shifted)
    labels = jnp.searchsorted(jnp.cumsum(tallies), jnp.arange(rows * top), side="right").astype(jnp.int32)
    grid = labels.reshape(top, rows).T
    grid = grid[jax.random.permutation(jax.random.fold_in(own, 1), rows)]
    rotation = jax.random.randint(jax.random.fold_in(own, 2), (rows, 1), 0, top)
    return jnp.take_along_axis(grid, (jnp.arange(top)[None, :] + rotation) % top, axis=1)


def load_shares(amount, total, most, slope, full):
    weights = [(1 << 20) // math.isqrt(standing ** slope) + 1 for standing in range(1, amount + 1)]
    largest = most if full else min(most, max(-(-total // amount), total * weights[0] // sum(weights)))
    least = 1 if total - largest >= amount - 1 else 0
    counts, surplus = [largest] + [least] * (amount - 1), total - largest - least * (amount - 1)
    while surplus > 0:
        movable = [i for i in range(1, amount) if counts[i] < largest] or [i for i in range(1, amount) if counts[i] < most]
        mass, remaining = sum([weights[i] for i in movable]), surplus
        for i in movable:
            more = min(most - counts[i], max(1, remaining * weights[i] // mass), surplus)
            counts[i] = counts[i] + more
            surplus = surplus - more
    return np.array(counts)


def gaussian(rng, shape, scale, most, shards=(), held_as=jnp.bfloat16):
    level = block_levels(rng, shape, shards, -0.22, 0.18) if shards else 1.0
    result = jax.random.normal(rng, shape, jnp.float32) * scale * level
    return jnp.minimum(jnp.maximum(result, -most), most).astype(held_as)


def setup_inputs(seed: int = 0) -> dict:
    streams_of = jax.random.split(jax.random.key(seed), 10)
    trajectory = gaussian(streams_of[0], (SECTIONS, NLAT, LEV, NLON), 1.0, 6.0, ((0, 4), (1, 8)), jnp.float32)
    diffusivity = jnp.clip(jnp.exp(math.log(0.24) - 2.4849066 * jax.random.uniform(streams_of[1], (SECTIONS, NLAT, LEV, NLON), jnp.float32) ** block_levels(streams_of[1], (SECTIONS, NLAT, LEV, NLON), ((0, 4), (1, 8)), -0.2, 0.2)), 0.02, 0.24)
    adjoint_end = gaussian(streams_of[2], (NLAT, LEV, NLON), 1.0, 6.0, ((0, 8),))
    obs_jac = gaussian(streams_of[3], (NOBS, CH, TILE), TILE ** -0.5, 0.5, ((0, 32),))
    obs_value = gaussian(streams_of[4], (NOBS, CH), 1.0, 6.0, ((0, 32),), jnp.float32)
    obs_weight = jnp.clip(jnp.exp(math.log(3.0) - 2.3025851 * jax.random.uniform(streams_of[5], (NOBS, CH), jnp.float32) ** block_levels(streams_of[5], (NOBS, CH), ((0, 32),), -0.2, 0.2)), 0.3, 3.0)
    obs_valid = with_ends((jax.random.randint(streams_of[6], (NOBS, CH), 0, 4) < 3).astype(jnp.int32), jax.random.fold_in(streams_of[6], 1), 0, 1)
    obs_owner_keys = jax.random.split(jax.random.fold_in(streams_of[7], 1), NOBS // NB_DEV)
    obs_owner_turns = jax.random.permutation(jax.random.fold_in(streams_of[7], 3), NOBS // NB_DEV)
    obs_owner = jax.vmap(lambda own, number: deal_out(jax.random.fold_in(streams_of[7], 2), own, number, NB_DEV, DEVICES, 1, CAP, 2))(obs_owner_keys, obs_owner_turns).reshape((NOBS, 1))
    obs_tile = with_ends(jax.random.randint(streams_of[8], (NOBS,), 0, TILES_DEV), jax.random.fold_in(streams_of[8], 1), 0, TILES_DEV - 1).astype(jnp.int32)
    return dict(trajectory=trajectory, diffusivity=diffusivity, adjoint_end=adjoint_end, obs_jac=obs_jac, obs_value=obs_value, obs_weight=obs_weight, obs_valid=obs_valid, obs_owner=obs_owner, obs_tile=obs_tile)


def spread(weighted):
    padded = jnp.pad(weighted, ((1, 1), (0, 0), (0, 0)))
    return padded[2:] + padded[:-2] + jnp.roll(weighted, 1, 2) + jnp.roll(weighted, -1, 2) - 4.0 * weighted


def propagate(field, kappa):
    for _ in range(SUB):
        field = field + spread(kappa * field)
    return field


def reference(trajectory, diffusivity, adjoint_end, obs_jac, obs_value, obs_weight, obs_valid, obs_owner, obs_tile):
    per_row = NLON // TW
    tiles = trajectory.reshape(SECTIONS, NLAT, LEV, per_row, TW).transpose(0, 1, 3, 2, 4).reshape(SECTIONS * NLAT * per_row, TILE)
    owner = obs_owner[:, 0]
    section = owner // N_LAT
    band = owner % N_LAT
    flat = (section * NLAT * per_row + band * TILES_DEV + obs_tile).astype(jnp.int32)
    states = tiles[flat]
    weights = obs_weight * obs_valid.astype(jnp.float32)

    def one(args):
        jac, state, value, weight = args
        jac_f = jac.astype(jnp.float32)
        pred = jnp.einsum("bct,bt->bc", jac_f, state, precision=lax.Precision.HIGHEST)
        resid = weight * (value - pred)
        return jnp.einsum("bct,bc->bt", jac_f, resid, precision=lax.Precision.HIGHEST)

    terms = lax.map(one, (obs_jac.reshape(DEVICES, NB_DEV, CH, TILE), states.reshape(DEVICES, NB_DEV, TILE),
                          obs_value.reshape(DEVICES, NB_DEV, CH), weights.reshape(DEVICES, NB_DEV, CH)))
    terms = terms.reshape(NOBS, TILE)
    forcing = jnp.zeros((SECTIONS * NLAT * per_row, TILE), jnp.float32).at[flat].add(terms)
    forcing = forcing.reshape(SECTIONS, NLAT, per_row, LEV, TW).transpose(0, 1, 3, 2, 4).reshape(SECTIONS, NLAT, LEV, NLON)
    results = [None] * SECTIONS
    current = adjoint_end.astype(jnp.float32)
    for section_id in range(SECTIONS - 1, -1, -1):
        if section_id == SECTIONS - 1:
            incoming = adjoint_end.astype(jnp.float32)
        else:
            incoming = lax.optimization_barrier(current.astype(jnp.bfloat16)).astype(jnp.float32)
        current = forcing[section_id] + propagate(incoming, diffusivity[section_id])
        results[section_id] = current
    return jnp.stack(results)
```

```python
import jax
import jax.numpy as jnp
from jax import lax
from jax.experimental import pallas as pl
from jax.experimental.pallas import tpu as pltpu
from jax.sharding import PartitionSpec as P

TW = 2
SUB = 2
LANES = 128
F32 = jnp.float32
BF16 = jnp.bfloat16
COEFF = jnp.float16

SMEM = pl.BlockSpec(memory_space=pltpu.SMEM)
VMEM = pl.BlockSpec(memory_space=pltpu.VMEM)


def route(owner, tile, sections, bands, slots):
    devices = sections * bands
    blocks = owner.shape[0]
    per_target = sections * slots

    def body(owner_ref, tile_ref, slot_ref, table_ref, used_ref):
        def clear(i, c):
            for j in range(per_target):
                table_ref[i * per_target + j] = -1
            used_ref[i] = 0
            return c

        lax.fori_loop(0, devices, clear, 0)

        def put(k, c):
            target = owner_ref[k]
            rank = used_ref[target]
            used_ref[target] = rank + 1
            slot_ref[k] = target * slots + rank
            section = target // bands
            band = target % bands
            for other in range(sections):
                at = ((other * bands + band) * sections + section) * slots + rank
                table_ref[at] = tile_ref[k]
            return c

        lax.fori_loop(0, blocks, put, 0)

    return pl.pallas_call(
        body,
        name="route",
        in_specs=[SMEM, SMEM],
        out_specs=[SMEM, SMEM],
        out_shape=[
            jax.ShapeDtypeStruct((blocks,), jnp.int32),
            jax.ShapeDtypeStruct((devices * per_target,), jnp.int32),
        ],
        scratch_shapes=[pltpu.SMEM((devices,), jnp.int32)],
    )(owner, tile)


def fetch_states(place, ids, traj, sections, slots):
    rows, levels, nlon = traj.shape
    per_row = nlon // TW
    pairs = LANES // TW
    per_target = sections * slots
    count = ids.shape[0] // sections

    def body(place_ref, ids_ref, traj_ref, out_ref, pairs_ref):
        lane = lax.broadcasted_iota(jnp.int32, (levels, LANES), 1)
        which = lax.broadcasted_iota(jnp.int32, (levels, LANES), 0)
        pick = (lane // TW == which).astype(BF16)
        mine = place_ref[0] * slots

        for group in range(count // pairs):

            def one(k, gathered):
                i = group * pairs + k
                at = (i // slots) * per_target + mine + i % slots
                tile = jnp.maximum(ids_ref[at], 0)
                row = tile // per_row
                column = tile % per_row
                start = pl.multiple_of(column // pairs * LANES, LANES)
                shift = (TW * k + LANES - column % pairs * TW) % LANES
                turned = pltpu.roll(traj_ref[row, :, pl.ds(start, LANES)], shift, 1)
                return jnp.where(lane // TW == k, turned, gathered)

            gathered = lax.fori_loop(
                0, pairs, one, jnp.zeros((levels, LANES), F32), unroll=8
            )
            pairs_ref[...] = sum(
                lax.dot_general(
                    piece.astype(BF16), pick, (((0,), (0,)), ((), ())),
                    preferred_element_type=F32,
                )
                for piece in split3(gathered)
            )
            even = pairs_ref[pl.ds(0, pairs, stride=TW), :]
            odd = pairs_ref[pl.ds(1, pairs, stride=TW), :]
            out_ref[group * pairs : (group + 1) * pairs, :] = jnp.where(
                lane[:pairs] % TW == 0, even, odd
            )

    return pl.pallas_call(
        body,
        name="fetch_states",
        in_specs=[SMEM, SMEM, VMEM],
        out_specs=VMEM,
        out_shape=jax.ShapeDtypeStruct((count, LANES), F32),
        scratch_shapes=[pltpu.VMEM((LANES, LANES), F32)],
    )(place, ids, traj)


def split3(x):
    a = x.astype(BF16).astype(F32)
    r = x - a
    b = r.astype(BF16).astype(F32)
    return a, b, r - b


def block_terms(slot, jac, found, value, weight, valid, sections, slots):
    blocks, channels, entries = jac.shape
    count = found.shape[0]
    part = LANES // sections
    group = 24 if blocks % 24 == 0 else blocks
    steps = blocks // group
    band_rows = count // sections

    def stacked(parts, k, which):
        picked = jnp.where(
            which == 0,
            jnp.broadcast_to(parts[0][k : k + 1], which.shape),
            jnp.where(
                which == 1,
                jnp.broadcast_to(parts[1][k : k + 1], which.shape),
                jnp.where(
                    which == 2, jnp.broadcast_to(parts[2][k : k + 1], which.shape), 0.0
                ),
            ),
        )
        return picked.astype(BF16)

    def body(slot_ref, jac_ref, found_ref, value_ref, weight_ref, valid_ref, out_ref, placed_ref, rows_ref):
        step = pl.program_id(0)
        which = lax.broadcasted_iota(jnp.int32, (16, LANES), 0)

        @pl.when(step == 0)
        def _():
            placed_ref[...] = jnp.zeros_like(placed_ref)

        base = step * group
        for k in range(group):
            rows_ref[k : k + 1, :] = found_ref[pl.ds(slot_ref[base + k], 1), :]
        state = split3(rows_ref[...])
        preds = []
        for k in range(group):
            got = lax.dot_general(
                stacked(state, k, which), jac_ref[k], (((1,), (1,)), ((), ())),
                preferred_element_type=F32,
            )
            preds.append(jnp.sum(got, axis=0, keepdims=True))
        pred = jnp.concatenate(preds, axis=0)
        gain = weight_ref[...] * valid_ref[...].astype(F32)
        resid = split3(gain * (value_ref[...] - pred))
        for k in range(group):
            got = lax.dot_general(
                stacked(resid, k, which), jac_ref[k], (((1,), (0,)), ((), ())),
                preferred_element_type=F32,
            )
            placed_ref[pl.ds(slot_ref[base + k], 1), :] = jnp.sum(got, axis=0, keepdims=True)

        @pl.when(step == steps - 1)
        def _():
            lane = lax.broadcasted_iota(jnp.int32, (band_rows, LANES), 1)
            for j in range(sections):
                total = jnp.zeros((band_rows, LANES), F32)
                for s in range(sections):
                    rows = placed_ref[s * band_rows : (s + 1) * band_rows, :]
                    shift = part * (s - j) % LANES
                    moved = pltpu.roll(rows, shift, 1) if shift else rows
                    total = jnp.where(lane // part == s, moved, total)
                out_ref[j * band_rows : (j + 1) * band_rows, :] = total

    rows_of = pl.BlockSpec((group, channels), lambda i: (i, 0))
    whole = pl.BlockSpec((count, LANES), lambda i: (0, 0))
    return pl.pallas_call(
        body,
        name="block_terms",
        grid=(steps,),
        in_specs=[
            SMEM,
            pl.BlockSpec((group, channels, entries), lambda i: (i, 0, 0)),
            whole,
            rows_of,
            rows_of,
            rows_of,
        ],
        out_specs=whole,
        out_shape=jax.ShapeDtypeStruct((count, LANES), F32),
        scratch_shapes=[pltpu.VMEM((count, LANES), F32), pltpu.VMEM((group, LANES), F32)],
    )(slot, jac, found, value, weight, valid)


def spread_forcing(ids, received, section, sections, slots, shape):
    rows, share, nlon = shape
    per_row = nlon // TW
    pairs = LANES // TW
    per_target = sections * slots
    count = received.shape[0]
    first = section * (LANES // sections)

    def body(ids_ref, recv_ref, out_ref, pairs_ref, terms_ref):
        out_ref[...] = jnp.zeros_like(out_ref)
        lane = lax.broadcasted_iota(jnp.int32, (share, LANES), 1)
        level = lax.broadcasted_iota(jnp.int32, (share, LANES), 0)
        pick = (lane // TW == level + first // TW).astype(BF16)
        parity = lax.broadcasted_iota(jnp.int32, (pairs, LANES), 1) % TW
        for group in range(count // pairs):
            block = recv_ref[group * pairs : (group + 1) * pairs, :]
            for j in range(TW):
                pairs_ref[pl.ds(j, pairs, stride=TW), :] = jnp.where(
                    parity == j, block, 0.0
                )
            terms_ref[group] = sum(
                lax.dot_general(
                    pick, piece.astype(BF16), (((1,), (1,)), ((), ())),
                    preferred_element_type=F32,
                )
                for piece in split3(pairs_ref[...])
            )

        def one(i, c):
            at = (i // slots) * per_target + section * slots + i % slots
            tile = jnp.maximum(ids_ref[at], 0)
            row = tile // per_row
            column = tile % per_row
            start = pl.multiple_of(column // pairs * LANES, LANES)
            off = column % pairs
            shift = (off + pairs - i % pairs) % pairs * TW
            turned = pltpu.roll(terms_ref[i // pairs], shift, 1)
            out_ref[row, :, pl.ds(start, LANES)] += jnp.where(
                lane // TW == off, turned, 0.0
            )
            return c

        lax.fori_loop(0, count, one, 0, unroll=8)

    return pl.pallas_call(
        body,
        name=f"spread_forcing_{section}",
        in_specs=[SMEM, VMEM],
        out_specs=VMEM,
        out_shape=jax.ShapeDtypeStruct(shape, F32),
        scratch_shapes=[
            pltpu.VMEM((LANES, LANES), F32),
            pltpu.VMEM((count // pairs, share, LANES), F32),
        ],
    )(ids, received)


def sweep(held, low, high, coeff, coeff_low, coeff_high, forcing, section):
    rows, share, nlon = held.shape
    halo = SUB

    def body(held_ref, low_ref, high_ref, c_ref, cl_ref, ch_ref, f_ref, out_ref):
        def of(own, lower, upper, r):
            if r < 0:
                return lower[r + halo].astype(F32)
            if r >= rows:
                return upper[r - rows].astype(F32)
            return own[r].astype(F32)

        field = {r: of(held_ref, low_ref, high_ref, r) for r in range(-halo, rows + halo)}
        for step in range(SUB):
            edge = halo - step
            weighted = {
                r: of(c_ref.at[0], cl_ref.at[0], ch_ref.at[0], r) * field[r]
                for r in range(-edge, rows + edge)
            }
            field = {
                r: field[r]
                + weighted[r + 1]
                + weighted[r - 1]
                + pltpu.roll(weighted[r], 1, 1)
                + pltpu.roll(weighted[r], nlon - 1, 1)
                - 4.0 * weighted[r]
                for r in range(-edge + 1, rows + edge - 1)
            }
        for r in range(rows):
            out_ref[r] = (f_ref[r] + field[r]).astype(out_ref.dtype)

    def full(shape):
        return pl.BlockSpec(shape, lambda i: (0,) * len(shape))

    def pick(shape):
        return pl.BlockSpec((1,) + shape[1:], lambda i: (section, 0, 0, 0))

    return pl.pallas_call(
        body,
        name=f"sweep_{section}",
        grid=(1,),
        in_specs=[
            full(held.shape), full(low.shape), full(high.shape),
            pick(coeff.shape), pick(coeff_low.shape), pick(coeff_high.shape),
            full(forcing.shape),
        ],
        out_specs=full(held.shape),
        out_shape=jax.ShapeDtypeStruct(held.shape, BF16),
    )(held, low, high, coeff, coeff_low, coeff_high, forcing)


def edges(block, dim, width):
    count = lax.axis_size("lat")
    forward = [(i, i + 1) for i in range(count - 1)]
    backward = [(j, i) for i, j in forward]
    size = block.shape[dim]
    low = lax.ppermute(lax.slice_in_dim(block, size - width, size, axis=dim), "lat", forward)
    high = lax.ppermute(lax.slice_in_dim(block, 0, width, axis=dim), "lat", backward)
    return low, high


def per_device(
    trajectory,
    diffusivity,
    adjoint_end,
    obs_jac,
    obs_value,
    obs_weight,
    obs_valid,
    obs_owner,
    obs_tile,
):
    traj = trajectory[0]
    rows, levels, nlon = traj.shape
    sections = lax.axis_size("tm")
    bands = lax.axis_size("lat")
    devices = sections * bands
    blocks = obs_owner.shape[0]
    slots = max(2, 2 * blocks // devices)
    share = levels // sections
    me = lax.axis_index("tm")
    every = ("tm", "lat")

    def exchange(x):
        return lax.all_to_all(x, every, split_axis=0, concat_axis=0, tiled=True)

    coeff = lax.all_to_all(
        diffusivity[0].astype(COEFF).reshape(rows, sections, share, nlon), "tm", 1, 0
    )
    coeff_low, coeff_high = edges(coeff, 1, SUB)
    coeff, coeff_low, coeff_high = (c.astype(F32) for c in (coeff, coeff_low, coeff_high))
    held = lax.dynamic_slice_in_dim(adjoint_end, me * share, share, axis=1)

    slot, table = route(obs_owner.reshape(blocks), obs_tile, sections, bands, slots)
    ids = exchange(table.reshape(devices, sections * slots)).reshape(-1)
    asked = fetch_states(me.astype(jnp.int32).reshape(1), ids, traj, sections, slots)
    found = exchange(asked.reshape(devices, slots, LANES)).reshape(devices * slots, LANES)
    terms = block_terms(
        slot, obs_jac, found, obs_value, obs_weight, obs_valid, sections, slots
    )
    received = exchange(terms.reshape(devices, slots, LANES)).reshape(devices * slots, LANES)

    results = [None] * sections
    for section in reversed(range(sections)):
        low, high = edges(held, 0, SUB)
        forcing = spread_forcing(
            ids, received, section, sections, slots, (rows, share, nlon)
        )
        held = sweep(held, low, high, coeff, coeff_low, coeff_high, forcing, section)
        results[section] = held
    mine = lax.all_to_all(jnp.stack(results), "tm", 0, 1)
    return mine.reshape(1, rows, levels, nlon).astype(F32)


def solution(mesh):
    in_specs = (
        P("tm", "lat", None, None),
        P("tm", "lat", None, None),
        P("lat", None, None),
        P(("tm", "lat"), None, None),
        P(("tm", "lat"), None),
        P(("tm", "lat"), None),
        P(("tm", "lat"), None),
        P(("tm", "lat"), None),
        P(("tm", "lat")),
    )
    out_specs = P("tm", "lat", None, None)
    return jax.shard_map(
        per_device, mesh=mesh, in_specs=in_specs, out_specs=out_specs, check_vma=False
    )
```

```python
import jax
import jax.numpy as jnp
from jax import lax
from jax.experimental import pallas as pl
from jax.experimental.pallas import tpu as pltpu
from jax.sharding import PartitionSpec as P

TW = 2
SUB = 2
LANES = 128
F32 = jnp.float32
BF16 = jnp.bfloat16
COEFF = jnp.float16

SMEM = pl.BlockSpec(memory_space=pltpu.SMEM)
VMEM = pl.BlockSpec(memory_space=pltpu.VMEM)


def split_index(x, n):
    if n & (n - 1):
        return x // n, x % n
    return lax.shift_right_logical(x, n.bit_length() - 1), lax.bitwise_and(x, n - 1)


def route(owner, tile, sections, bands, slots):
    devices = sections * bands
    blocks = owner.shape[0]
    per_target = sections * slots

    def body(owner_ref, tile_ref, slot_ref, table_ref, used_ref):
        def clear(i, c):
            for j in range(per_target):
                table_ref[i * per_target + j] = -1
            used_ref[i] = 0
            return c

        lax.fori_loop(0, devices, clear, 0)

        def put(k, c):
            target = owner_ref[k]
            rank = used_ref[target]
            used_ref[target] = rank + 1
            slot_ref[k] = target * slots + rank
            section, band = split_index(target, bands)
            tile = tile_ref[k]
            for other in range(sections):
                at = ((other * bands + band) * sections + section) * slots + rank
                table_ref[at] = tile
            return c

        lax.fori_loop(0, blocks, put, 0)

    return pl.pallas_call(
        body,
        name="route",
        in_specs=[SMEM, SMEM],
        out_specs=[SMEM, SMEM],
        out_shape=[
            jax.ShapeDtypeStruct((blocks,), jnp.int32),
            jax.ShapeDtypeStruct((devices * per_target,), jnp.int32),
        ],
        scratch_shapes=[pltpu.SMEM((devices,), jnp.int32)],
    )(owner, tile)


def fetch_states(place, ids, traj, sections, slots):
    rows, levels, nlon = traj.shape
    per_row = nlon // TW
    pairs = LANES // TW
    per_target = sections * slots
    count = ids.shape[0] // sections
    devices = count // slots
    run = min(devices, pairs)

    def body(place_ref, ids_ref, traj_ref, out_ref, pairs_ref):
        lane = lax.broadcasted_iota(jnp.int32, (levels, LANES), 1)
        which = lax.broadcasted_iota(jnp.int32, (levels, LANES), 0)
        pick = (lane // TW == which).astype(BF16)
        mine = place_ref[0] * slots

        for group in range(count // pairs):

            def one(k, gathered):
                slot, device = split_index(group * pairs + k, devices)
                tile = jnp.maximum(ids_ref[device * per_target + mine + slot], 0)
                row, column = split_index(tile, per_row)
                block, off = split_index(column, pairs)
                start = pl.multiple_of(block * LANES, LANES)
                shift = lax.bitwise_and(TW * (k + pairs - off), LANES - 1)
                turned = pltpu.roll(traj_ref[row, :, pl.ds(start, LANES)], shift, 1)
                return jnp.where(lane // TW == k, turned, gathered)

            gathered = lax.fori_loop(
                0, pairs, one, jnp.zeros((levels, LANES), F32), unroll=16
            )
            pairs_ref[...] = sum(
                lax.dot_general(
                    piece.astype(BF16), pick, (((0,), (0,)), ((), ())),
                    preferred_element_type=F32,
                )
                for piece in split3(gathered)
            )
            even = pairs_ref[pl.ds(0, pairs, stride=TW), :]
            odd = pairs_ref[pl.ds(1, pairs, stride=TW), :]
            both = jnp.where(lane[:pairs] % TW == 0, even, odd)
            for j in range(pairs // run):
                slot, device = divmod(group * pairs + j * run, devices)
                out_ref[pl.ds(device * slots + slot, run, stride=slots), :] = both[
                    j * run : (j + 1) * run
                ]

    return pl.pallas_call(
        body,
        name="fetch_states",
        in_specs=[SMEM, SMEM, VMEM],
        out_specs=VMEM,
        out_shape=jax.ShapeDtypeStruct((count, LANES), F32),
        scratch_shapes=[pltpu.VMEM((LANES, LANES), F32)],
    )(place, ids, traj)


def split3(x):
    a = x.astype(BF16).astype(F32)
    r = x - a
    b = r.astype(BF16).astype(F32)
    return a, b, r - b


def block_terms(slot, jac, found, value, weight, valid, sections, slots):
    blocks, channels, entries = jac.shape
    count = found.shape[0]
    part = LANES // sections
    group = 24 if blocks % 24 == 0 else blocks
    steps = blocks // group
    band_rows = count // sections

    def stacked(parts, k, which):
        picked = jnp.where(
            which == 0,
            jnp.broadcast_to(parts[0][k : k + 1], which.shape),
            jnp.where(
                which == 1,
                jnp.broadcast_to(parts[1][k : k + 1], which.shape),
                jnp.where(
                    which == 2, jnp.broadcast_to(parts[2][k : k + 1], which.shape), 0.0
                ),
            ),
        )
        return picked.astype(BF16)

    def body(slot_ref, jac_ref, found_ref, value_ref, weight_ref, valid_ref, out_ref, placed_ref, rows_ref):
        step = pl.program_id(0)
        which = lax.broadcasted_iota(jnp.int32, (16, LANES), 0)

        @pl.when(step == 0)
        def _():
            placed_ref[...] = jnp.zeros_like(placed_ref)

        base = step * group
        for k in range(group):
            rows_ref[k : k + 1, :] = found_ref[pl.ds(slot_ref[base + k], 1), :]
        state = split3(rows_ref[...])
        preds = []
        for k in range(group):
            got = lax.dot_general(
                stacked(state, k, which), jac_ref[k], (((1,), (1,)), ((), ())),
                preferred_element_type=F32,
            )
            preds.append(jnp.sum(got, axis=0, keepdims=True))
        pred = jnp.concatenate(preds, axis=0)
        gain = weight_ref[...] * valid_ref[...].astype(F32)
        resid = split3(gain * (value_ref[...] - pred))
        for k in range(group):
            got = lax.dot_general(
                stacked(resid, k, which), jac_ref[k], (((1,), (0,)), ((), ())),
                preferred_element_type=F32,
            )
            placed_ref[pl.ds(slot_ref[base + k], 1), :] = jnp.sum(got, axis=0, keepdims=True)

        @pl.when(step == steps - 1)
        def _():
            lane = lax.broadcasted_iota(jnp.int32, (band_rows, LANES), 1)
            for j in range(sections):
                total = jnp.zeros((band_rows, LANES), F32)
                for s in range(sections):
                    rows = placed_ref[s * band_rows : (s + 1) * band_rows, :]
                    shift = part * (s - j) % LANES
                    moved = pltpu.roll(rows, shift, 1) if shift else rows
                    total = jnp.where(lane // part == s, moved, total)
                out_ref[j * band_rows : (j + 1) * band_rows, :] = total

    rows_of = pl.BlockSpec((group, channels), lambda i: (i, 0))
    whole = pl.BlockSpec((count, LANES), lambda i: (0, 0))
    return pl.pallas_call(
        body,
        name="block_terms",
        grid=(steps,),
        in_specs=[
            SMEM,
            pl.BlockSpec((group, channels, entries), lambda i: (i, 0, 0)),
            whole,
            rows_of,
            rows_of,
            rows_of,
        ],
        out_specs=whole,
        out_shape=jax.ShapeDtypeStruct((count, LANES), F32),
        scratch_shapes=[pltpu.VMEM((count, LANES), F32), pltpu.VMEM((group, LANES), F32)],
    )(slot, jac, found, value, weight, valid)


def spread_forcing(ids, received, section, sections, slots, shape):
    rows, share, nlon = shape
    per_row = nlon // TW
    pairs = LANES // TW
    per_target = sections * slots
    count = received.shape[0]
    first = section * (LANES // sections)

    heaps = min(slots, 3)

    def body(ids_ref, recv_ref, out_ref, pairs_ref, terms_ref, *heap_refs):
        heap_refs = (out_ref,) + heap_refs
        for ref in heap_refs:
            ref[...] = jnp.zeros_like(ref)
        lane = lax.broadcasted_iota(jnp.int32, (share, LANES), 1)
        level = lax.broadcasted_iota(jnp.int32, (share, LANES), 0)
        pick = (lane // TW == level + first // TW).astype(BF16)
        parity = lax.broadcasted_iota(jnp.int32, (pairs, LANES), 1) % TW
        for group in range(count // pairs):
            block = recv_ref[group * pairs : (group + 1) * pairs, :]
            for j in range(TW):
                pairs_ref[pl.ds(j, pairs, stride=TW), :] = jnp.where(
                    parity == j, block, 0.0
                )
            terms_ref[group] = sum(
                lax.dot_general(
                    pick, piece.astype(BF16), (((1,), (1,)), ((), ())),
                    preferred_element_type=F32,
                )
                for piece in split3(pairs_ref[...])
            )

        def one(device, c):
            for slot in range(slots):
                tile = jnp.maximum(
                    ids_ref[device * per_target + section * slots + slot], 0
                )
                group, k = split_index(device * slots + slot, pairs)
                row, column = split_index(tile, per_row)
                at, off = split_index(column, pairs)
                start = pl.multiple_of(at * LANES, LANES)
                shift = lax.bitwise_and(off + pairs - k, pairs - 1) * TW
                turned = pltpu.roll(terms_ref[group], shift, 1)
                heap_refs[slot % heaps][row, :, pl.ds(start, LANES)] += jnp.where(
                    lane // TW == off, turned, 0.0
                )
            return c

        lax.fori_loop(0, count // slots, one, 0, unroll=2)
        out_ref[...] = sum(ref[...] for ref in heap_refs[1:]) + out_ref[...]

    return pl.pallas_call(
        body,
        name=f"spread_forcing_{section}",
        in_specs=[SMEM, VMEM],
        out_specs=VMEM,
        out_shape=jax.ShapeDtypeStruct(shape, F32),
        scratch_shapes=[
            pltpu.VMEM((LANES, LANES), F32),
            pltpu.VMEM((count // pairs, share, LANES), F32),
        ]
        + [pltpu.VMEM(shape, F32)] * (heaps - 1),
    )(ids, received)


def sweep(held, low, high, coeff, coeff_low, coeff_high, forcing, section):
    rows, share, nlon = held.shape
    halo = SUB

    def body(held_ref, low_ref, high_ref, c_ref, cl_ref, ch_ref, f_ref, out_ref):
        def of(own, lower, upper, r):
            if r < 0:
                return lower[r + halo].astype(F32)
            if r >= rows:
                return upper[r - rows].astype(F32)
            return own[r].astype(F32)

        field = {r: of(held_ref, low_ref, high_ref, r) for r in range(-halo, rows + halo)}
        for step in range(SUB):
            edge = halo - step
            weighted = {
                r: of(c_ref.at[0], cl_ref.at[0], ch_ref.at[0], r) * field[r]
                for r in range(-edge, rows + edge)
            }
            field = {
                r: field[r]
                + weighted[r + 1]
                + weighted[r - 1]
                + pltpu.roll(weighted[r], 1, 1)
                + pltpu.roll(weighted[r], nlon - 1, 1)
                - 4.0 * weighted[r]
                for r in range(-edge + 1, rows + edge - 1)
            }
        for r in range(rows):
            out_ref[r] = (f_ref[r] + field[r]).astype(out_ref.dtype)

    def full(shape):
        return pl.BlockSpec(shape, lambda i: (0,) * len(shape))

    def pick(shape):
        return pl.BlockSpec((1,) + shape[1:], lambda i: (section, 0, 0, 0))

    return pl.pallas_call(
        body,
        name=f"sweep_{section}",
        grid=(1,),
        in_specs=[
            full(held.shape), full(low.shape), full(high.shape),
            pick(coeff.shape), pick(coeff_low.shape), pick(coeff_high.shape),
            full(forcing.shape),
        ],
        out_specs=full(held.shape),
        out_shape=jax.ShapeDtypeStruct(held.shape, BF16),
    )(held, low, high, coeff, coeff_low, coeff_high, forcing)


def edges(block, dim, width):
    count = lax.axis_size("lat")
    forward = [(i, i + 1) for i in range(count - 1)]
    backward = [(j, i) for i, j in forward]
    size = block.shape[dim]
    low = lax.ppermute(lax.slice_in_dim(block, size - width, size, axis=dim), "lat", forward)
    high = lax.ppermute(lax.slice_in_dim(block, 0, width, axis=dim), "lat", backward)
    return low, high


def per_device(
    trajectory,
    diffusivity,
    adjoint_end,
    obs_jac,
    obs_value,
    obs_weight,
    obs_valid,
    obs_owner,
    obs_tile,
):
    traj = trajectory[0]
    rows, levels, nlon = traj.shape
    sections = lax.axis_size("tm")
    bands = lax.axis_size("lat")
    devices = sections * bands
    blocks = obs_owner.shape[0]
    slots = max(2, 2 * blocks // devices)
    share = levels // sections
    me = lax.axis_index("tm")
    every = ("tm", "lat")

    def exchange(x):
        return lax.all_to_all(x, every, split_axis=0, concat_axis=0, tiled=True)

    coeff = lax.all_to_all(
        diffusivity[0].astype(COEFF).reshape(rows, sections, share, nlon), "tm", 1, 0
    )
    coeff_low, coeff_high = edges(coeff, 1, SUB)
    coeff, coeff_low, coeff_high = (c.astype(F32) for c in (coeff, coeff_low, coeff_high))
    held = lax.dynamic_slice_in_dim(adjoint_end, me * share, share, axis=1)

    slot, table = route(obs_owner.reshape(blocks), obs_tile, sections, bands, slots)
    ids = exchange(table.reshape(devices, sections * slots)).reshape(-1)
    asked = fetch_states(me.astype(jnp.int32).reshape(1), ids, traj, sections, slots)
    found = exchange(asked.reshape(devices, slots, LANES)).reshape(devices * slots, LANES)
    terms = block_terms(
        slot, obs_jac, found, obs_value, obs_weight, obs_valid, sections, slots
    )
    received = exchange(terms.reshape(devices, slots, LANES)).reshape(devices * slots, LANES)

    results = [None] * sections
    for section in reversed(range(sections)):
        low, high = edges(held, 0, SUB)
        forcing = spread_forcing(
            ids, received, section, sections, slots, (rows, share, nlon)
        )
        held = sweep(held, low, high, coeff, coeff_low, coeff_high, forcing, section)
        results[section] = held
    mine = lax.all_to_all(jnp.stack(results), "tm", 0, 1)
    return mine.reshape(1, rows, levels, nlon).astype(F32)


def solution(mesh):
    in_specs = (
        P("tm", "lat", None, None),
        P("tm", "lat", None, None),
        P("lat", None, None),
        P(("tm", "lat"), None, None),
        P(("tm", "lat"), None),
        P(("tm", "lat"), None),
        P(("tm", "lat"), None),
        P(("tm", "lat"), None),
        P(("tm", "lat")),
    )
    out_specs = P("tm", "lat", None, None)
    return jax.shard_map(
        per_device, mesh=mesh, in_specs=in_specs, out_specs=out_specs, check_vma=False
    )
```
